32 devices in a mesh: section: 4 (over y, core), dp: 2 (over x), expert: 4 (over z).
Axes of the slice: x: 2, y: 2, z: 4, core: 2. Of those that a mesh axis runs over, the one named last changes fastest.
Arguments:
- inputs: bfloat16 [4, 1024, 2048], P('section', ('dp', 'expert')), may hold values from -6 to 6
- in_cache: bfloat16 [4, 1024, 2048], P('section', ('dp', 'expert')), may hold values from -6 to 6
- out_cache: bfloat16 [4, 1024, 2048], P('section', ('dp', 'expert')), may hold values from -6 to 6
- w_up: bfloat16 [4, 2048, 57344], P('section', None, ('dp', 'expert')), may hold values from -0.125 to 0.125
- w_down: bfloat16 [4, 57344, 2048], P('section', ('dp', 'expert')), may hold values from -0.0625 to 0.0625
- routing: int32 [4, 1024, 2], P('section', ('dp', 'expert')), may hold values from 0 to 7, all different within a row; in each aligned block of 128 rows (0 to 127, 128 to 255, ..., all dimensions but the last counted through in order) at most 32 rows name the same one
- gate_table: int32 [4, 1024, 2], P('section', ('dp', 'expert')), may hold values from 1 to 16
- lengths: int32 [64], P(('dp', 'expert')), may hold values from 1 to 16
- sample_map: int32 [64], replicated, may hold values from 0 to 63, as said below
Outputs:
- next_input: bfloat16 [4, 1024, 2048], P('section', ('dp', 'expert'))
- new_out_cache: bfloat16 [4, 1024, 2048], P('section', ('dp', 'expert'))
The draws below stay inside these ranges and needn't reach their ends.
Inputs may be any that keep to these rules, and one draw needn't show every extreme that they name: `sample_map`: A permutation. Every sample keeps its index along expert; the samples of one device go to exactly 2 replicas, exactly 4 to each. `routing`: A row names 2 different experts; in the rows of one device each expert is named exactly 32 times.
All inputs are finite; a program needn't handle non-finite values.
Results may differ from the reference program's by a relative error of at most 0.007.
Values may be sent and summed in bfloat16 or wider, within the bound.
A program may use at most 128 MiB of HBM per device.

```python
import math
import jax
import jax.numpy as jnp
import numpy as np
from jax import lax

D = 2048
FF = 7168
EXPERTS = 8
TOPK = 2
ROWS = 16
SAMP_DEV = 8
TOK_DEV = 128
SAMPLES = 64
TOKENS = 1024
CAP_E = 32
CAP_S = 4
N_SECTION = 4
N_DP = 2
N_EXPERT = 4


def shuffled_rows(row_key, count, length):
    return jax.vmap(lambda single_key: jax.random.permutation(single_key, length))(jax.random.split(row_key, count))


def draw_sample_map(key, part):
    block_count = SAMP_DEV // CAP_S
    columns = []
    for column in range(N_EXPERT):
        column_key = jax.random.fold_in(key, 101 + column)
        outer_perm = jax.random.permutation(jax.random.fold_in(column_key, 1), N_DP)
        inner_perm = jax.random.permutation(jax.random.fold_in(column_key, 2), N_DP)
        offsets = jax.random.permutation(jax.random.fold_in(column_key, 3), N_DP)[:block_count]
        turned = shuffled_rows(jax.random.fold_in(column_key, 4), N_DP, SAMP_DEV)
        settle = shuffled_rows(jax.random.fold_in(column_key, 5), N_DP, SAMP_DEV)
        block_ids = turned // CAP_S
        within = turned % CAP_S
        dest_rep = outer_perm[(inner_perm[:, None] + offsets[block_ids]) % N_DP]
        new_local = settle[dest_rep, block_ids * CAP_S + within]
        columns.append((dest_rep * N_EXPERT + column) * SAMP_DEV + new_local)
    stacked = jnp.stack(columns, axis=1)
    return stacked.reshape(SAMPLES).astype(jnp.int32)


def plant(array, stream_key, smallest, largest):
    shape = array.shape
    index_at = [jax.random.randint(jax.random.fold_in(stream_key, axis), (), 0, shape[axis]) for axis in range(len(shape))]
    array = array.at[tuple(index_at)].set(smallest)
    longest = shape.index(max(shape))
    index_at[longest] = (index_at[longest] + 1) % shape[longest]
    return array.at[tuple(index_at)].set(largest)


def block_levels(key, dims, cuts, low, top_value):
    factor_of = 1.0
    for dim, shards_of in cuts:
        draws = jax.random.uniform(jax.random.fold_in(jax.random.fold_in(key, 6), dim), (shards_of,), jnp.float32, low / len(cuts), top_value / len(cuts))
        factor_of = factor_of * jnp.repeat(jnp.exp(draws), dims[dim] // shards_of).reshape((-1,) + (1,) * (len(dims) - 1 - dim))
    return factor_of


def routed_block(own_key, own, number, rows, count, top, most, slope):
    sequence = jax.random.permutation(own_key, count)
    heavy_load, ordinary = shares(count, rows * top, most, slope, True), shares(count, rows * top, most, slope, False)
    places = jnp.arange(count)

    def named(sizes, offset_by):
        used = int((sizes > 0).sum())
        fixed = max(1, used // 4)
        passed = fixed + (places - fixed + offset_by * (used - fixed)) % max(1, count - fixed)
        return jnp.zeros((count,), jnp.int32).at[sequence[jnp.where(places < fixed, places, passed)]].set(jnp.asarray(sizes, jnp.int32))

    sizes = jnp.where(number % 4 == 0, named(heavy_load, number // 4), named(ordinary, number - number // 4 - 1))
    mixed = jax.random.permutation(jax.random.fold_in(own, 3), count)
    donor, sink = mixed[0:count // 2 * 2:2], mixed[1:count // 2 * 2:2]
    slack = jnp.minimum(sizes[donor] - 1, most - sizes[sink]) // 2
    slack = jnp.where((donor == sequence[0]) | (sink == sequence[0]) | (sizes[sink] == 0), 0, jnp.maximum(slack, 0))
    passed = jax.random.randint(jax.random.fold_in(own, 4), (count // 2,), 0, 1 << 20) % (slack + 1)
    sizes = sizes.at[donor].add(-passed).at[sink].add(passed)
    items = jnp.searchsorted(jnp.cumsum(sizes), jnp.arange(rows * top), side="right").astype(jnp.int32)
    listing = items.reshape(top, rows).T
    listing = listing[jax.random.permutation(jax.random.fold_in(own, 1), rows)]
    offset_by = jax.random.randint(jax.random.fold_in(own, 2), (rows, 1), 0, top)
    return jnp.take_along_axis(listing, (jnp.arange(top)[None, :] + offset_by) % top, axis=1)


def shares(number_of, total, most, skew, full):
    loads = [(1 << 20) // math.isqrt(grade ** skew) + 1 for grade in range(1, number_of + 1)]
    largest = most if full else min(most, max(-(-total // number_of), total * loads[0] // sum(loads)))
    least = 1 if total - largest >= number_of - 1 else 0
    holding, surplus = [largest] + [least] * (number_of - 1), total - largest - least * (number_of - 1)
    while surplus > 0:
        free = [i for i in range(1, number_of) if holding[i] < largest] or [i for i in range(1, number_of) if holding[i] < most]
        mass, remaining = sum([loads[i] for i in free]), surplus
        for i in free:
            more = min(most - holding[i], max(1, remaining * loads[i] // mass), surplus)
            holding[i] = holding[i] + more
            surplus = surplus - more
    return np.array(holding)


def scatter_about(own_key, dims, scale, most, cuts=(), held_as=jnp.bfloat16):
    result = scale * jax.random.normal(own_key, dims, jnp.float32)
    if cuts:
        result = result * block_levels(own_key, dims, cuts, -0.22, 0.18)
    return jnp.clip(result, -most, most).astype(held_as)


def setup_inputs(seed: int = 0) -> dict:
    key_of = jax.random.split(jax.random.key(seed), 10)
    inputs = scatter_about(key_of[0], (N_SECTION, TOKENS, D), 1.0, 6.0, ((0, 4), (1, 8)))
    in_cache = scatter_about(key_of[1], (N_SECTION, TOKENS, D), 1.0, 6.0, ((0, 4), (1, 8)))
    out_cache = scatter_about(key_of[2], (N_SECTION, TOKENS, D), 1.0, 6.0, ((0, 4), (1, 8)))
    w_up = scatter_about(key_of[3], (N_SECTION, D, EXPERTS * FF), D ** -0.5, 0.125, ((0, 4), (2, 8)))
    w_down = scatter_about(key_of[4], (N_SECTION, EXPERTS * FF, D), FF ** -0.5, 0.0625, ((0, 4), (1, 8)))
    routing_keys = jax.random.split(jax.random.fold_in(key_of[5], 1), N_SECTION * TOKENS // TOK_DEV)
    routing_turns = jax.random.permutation(jax.random.fold_in(key_of[5], 3), N_SECTION * TOKENS // TOK_DEV)
    routing = jax.vmap(lambda own, number: routed_block(jax.random.fold_in(key_of[5], 2), own, number, TOK_DEV, EXPERTS, TOPK, CAP_E, 0))(routing_keys, routing_turns).reshape((N_SECTION, TOKENS, TOPK))
    gate_table = plant(jax.random.randint(key_of[6], (N_SECTION, TOKENS, TOPK), 1, 17), jax.random.fold_in(key_of[6], 1), 1, 16).astype(jnp.int32)
    lengths = plant(jax.random.randint(key_of[7], (SAMPLES,), 1, ROWS + 1), jax.random.fold_in(key_of[7], 1), 1, ROWS).astype(jnp.int32)
    sample_map = draw_sample_map(jax.random.fold_in(key_of[9], 71), 0)
    return dict(inputs=inputs, in_cache=in_cache, out_cache=out_cache, w_up=w_up, w_down=w_down, routing=routing, gate_table=gate_table, lengths=lengths, sample_map=sample_map)


def reference(inputs, in_cache, out_cache, w_up, w_down, routing, gate_table, lengths, sample_map):
    feature_width = inputs.shape[2]
    total_samples = sample_map.shape[0]
    sources = jnp.zeros((total_samples,), jnp.int32).at[sample_map].set(jnp.arange(total_samples, dtype=jnp.int32))

    def migrate(cache):
        shaped = cache.reshape(N_SECTION, total_samples, ROWS, feature_width)
        return shaped[:, sources].reshape(N_SECTION, total_samples * ROWS, feature_width)

    in_moved = migrate(in_cache)
    out_moved = migrate(out_cache)
    slice_count = N_DP * N_EXPERT // EXPERTS
    slice_width = FF // slice_count
    per_expert = total_samples * ROWS * TOPK // EXPERTS

    def expert_layer(section_args):
        tokens, up_section, down_section, chosen, gates = section_args
        flat_experts = chosen.reshape(-1)
        sorted_order = jnp.argsort(flat_experts, stable=True).astype(jnp.int32)
        grouped = tokens[sorted_order // TOPK].reshape(EXPERTS, per_expert, feature_width)
        up_all = up_section.reshape(feature_width, EXPERTS, FF).transpose(1, 0, 2)
        down_all = down_section.reshape(EXPERTS, FF, feature_width)

        def one_expert(expert_args):
            rows_here, up_here, down_here = expert_args
            hidden = jax.nn.silu(jnp.dot(rows_here, up_here, preferred_element_type=jnp.float32)).astype(jnp.bfloat16)
            pieces = jnp.einsum("rsf,sfd->srd",
                                hidden.reshape(per_expert, slice_count, slice_width).astype(jnp.float32),
                                down_here.reshape(slice_count, slice_width, feature_width).astype(jnp.float32))
            rounded = lax.optimization_barrier(pieces.astype(jnp.bfloat16)).astype(jnp.float32)
            return jnp.sum(rounded, axis=0)

        expert_rows = lax.map(one_expert, (grouped, up_all, down_all)).reshape(-1, feature_width)
        position = jnp.zeros_like(sorted_order).at[sorted_order].set(jnp.arange(sorted_order.shape[0], dtype=jnp.int32))
        per_assign = expert_rows[position].reshape(tokens.shape[0], TOPK, feature_width)
        weights = gates.astype(jnp.float32)
        weights = weights / jnp.sum(weights, axis=1, keepdims=True)
        return jnp.sum(weights[:, :, None] * per_assign, axis=1)

    mixed = lax.map(expert_layer, (inputs, w_up, w_down, routing, gate_table))
    valid_rows = (jnp.arange(ROWS, dtype=jnp.int32)[None, :] < lengths[:, None]).reshape(-1)
    delta_rows = jnp.where(valid_rows[None, :, None], (mixed - out_moved.astype(jnp.float32)).astype(jnp.bfloat16), jnp.zeros((), jnp.bfloat16))
    new_out_cache = (out_moved.astype(jnp.float32) + delta_rows.astype(jnp.float32)).astype(jnp.bfloat16)
    received = jnp.concatenate([jnp.zeros_like(delta_rows[:1]), delta_rows[:-1]], axis=0)
    next_input = (in_moved.astype(jnp.float32) + received.astype(jnp.float32)).astype(jnp.bfloat16)
    return next_input, new_out_cache
```

```python
import functools

import jax
import jax.numpy as jnp
from jax import lax
from jax.experimental import pallas as pl
from jax.experimental.pallas import tpu as pltpu
from jax.sharding import PartitionSpec as P

EXPERTS = 8
TOPK = 2
ROWS = 16
SAMP_DEV = 8


def from_behind(value, axis, by):
    peers = lax.axis_size(axis)
    pairs = [(i, i + by) for i in range(peers) if 0 <= i + by < peers]
    return lax.ppermute(value, axis, pairs)


def cache_plan(sample_map, own_device, own_dp, dp_count, expert_count, cap_slots):
    total = sample_map.shape[0]
    ids = jnp.arange(total, dtype=jnp.int32)
    local = jnp.arange(SAMP_DEV, dtype=jnp.int32)
    own_map = lax.dynamic_slice_in_dim(sample_map, own_device * SAMP_DEV, SAMP_DEV)
    dest_dp = own_map // (SAMP_DEV * expert_count)
    slot = jnp.sum(
        ((dest_dp[:, None] == dest_dp[None, :]) & (local[None, :] < local[:, None])).astype(jnp.int32),
        axis=1,
    )
    places = jnp.arange(dp_count * cap_slots, dtype=jnp.int32)
    to_send = jnp.sum(
        jnp.where(places[:, None] == (dest_dp * cap_slots + slot)[None, :], local[None, :], 0), axis=1
    )
    wanted = own_device * SAMP_DEV + local
    sources = jnp.sum(jnp.where(sample_map[None, :] == wanted[:, None], ids[None, :], 0), axis=1)
    source_device = sources // SAMP_DEV
    earlier = (
        (ids[None, :] // SAMP_DEV == source_device[:, None])
        & (ids[None, :] < sources[:, None])
        & (sample_map[None, :] // (SAMP_DEV * expert_count) == own_dp)
    )
    arrival = source_device // expert_count * cap_slots + jnp.sum(earlier.astype(jnp.int32), axis=1)
    return to_send, arrival


def token_plan(routing, gate_table, per_expert):
    tok_rows = routing.shape[0]
    before = jnp.arange(tok_rows)[None, :] < jnp.arange(tok_rows)[:, None]
    weights = gate_table.astype(jnp.float32)
    weights = weights / jnp.sum(weights, axis=1, keepdims=True)
    slots = jnp.arange(EXPERTS * per_expert, dtype=jnp.int32)
    select, mix = 0, 0
    for k in range(TOPK):
        own = routing[:, k]
        rank = 0
        for j in range(TOPK):
            rank = rank + jnp.sum((before & (routing[:, j][None, :] == own[:, None])).astype(jnp.int32), axis=1)
        slot = own * per_expert + rank
        select = select + (slots[:, None] == slot[None, :]).astype(jnp.bfloat16)
        mix = mix + jnp.where(slots[None, :] == slot[:, None], weights[:, k][:, None], 0.0)
    return select, mix


UP_BLOCKS = 4
DOWN_BLOCKS = 4
KERNEL_VMEM = 67043328


def rows_iota(rows, columns, axis):
    return lax.broadcasted_iota(jnp.int32, (rows, columns), axis)


def token_slots(routing, own_dp, own_expert, expert_count, dp_count, per_expert):
    tok_rows = routing.shape[1]
    half, half_rows = expert_count // 2, per_expert // 2
    near_rows, chunk_rows = dp_count * half * per_expert, dp_count * half * half_rows
    names = rows_iota(16, tok_rows, 0)
    chosen = [routing[k : k + 1, :] for k in range(TOPK)]
    named = 0.0
    for own in chosen:
        named = named + jnp.where(names == own, 1.0, 0.0)
    before = jnp.where(rows_iota(tok_rows, tok_rows, 0) < rows_iota(tok_rows, tok_rows, 1), 1.0, 0.0)
    ranks = jnp.dot(named.astype(jnp.bfloat16), before.astype(jnp.bfloat16), preferred_element_type=jnp.float32)
    slots = []
    for own in chosen:
        rank = jnp.sum(jnp.where(names == own, ranks, 0.0), axis=0, keepdims=True).astype(jnp.int32)
        dd = lax.bitwise_xor(lax.div(own, expert_count), own_dp)
        m = lax.bitwise_xor(lax.rem(own, expert_count), own_expert)
        place = dd * half + lax.rem(m, half)
        late = jnp.where(rank >= half_rows, chunk_rows - half_rows, 0)
        far = near_rows + place * half_rows + rank + late
        slots.append(jnp.where(m < half, place * per_expert + rank, far))
    return slots


def sample_rows(sample_map, device, tok_rows, expert_count, to_dp):
    lane = rows_iota(1, tok_rows, 1)
    sample, within = lax.div(lane, ROWS), lax.rem(lane, ROWS)
    places, slots, used = jnp.zeros_like(lane), jnp.zeros_like(lane), 0
    for g in range(SAMP_DEV):
        place = sample_map[device * SAMP_DEV + g]
        goes = (lax.div(place, SAMP_DEV * expert_count) == to_dp).astype(jnp.int32)
        base = goes * (used * ROWS) - (1 - goes) * tok_rows
        places = jnp.where(sample == g, place, places)
        slots = jnp.where(sample == g, base, slots)
        used = used + goes
    return places, slots + within


def one_hot(mask):
    return jnp.where(mask, 1.0, 0.0).astype(jnp.bfloat16)


def section_kernel(
    dp_count, expert_count, section_count, per_expert,
    routing, gates, lengths, sample_map, inputs, in_cache, out_cache, w_up, w_down,
    out_moved, delta, in_moved, received,
    up_buf, down_buf, first, second, leaving, coming, grouped, arrived, hidden, returned, mix, own_pick, far_pick,
    up_sem, down_sem, load_sem, there_send, there_recv, back_send, back_recv,
    cache_send, cache_recv, store_sem, delta_store, delta_send, delta_recv,
):
    own_dp, own_expert, own_section = lax.axis_index("dp"), lax.axis_index("expert"), lax.axis_index("section")
    me = own_dp * expert_count + own_expert
    tok_rows, width = inputs.shape
    slots = tok_rows * TOPK
    ups, up_width = up_buf.shape[0], up_buf.shape[2]
    downs, down_width = down_buf.shape[0], down_buf.shape[2]
    half, half_rows = expert_count // 2, per_expert // 2
    group = dp_count * half
    near_rows, chunk_rows = group * per_expert, group * half_rows
    moved_rows = leaving.shape[1]
    mesh_id = pl.DeviceIdType.MESH

    near = [(dd, m) for dd in range(dp_count) for m in range(half)]
    far = [(dd, m + half) for dd in range(dp_count) for m in range(half)]
    pieces = [(i * per_expert, per_expert, peer) for i, peer in enumerate(near)][1:]
    for c in range(2):
        pieces += [(near_rows + c * chunk_rows + j * half_rows, half_rows, peer) for j, peer in enumerate(far)]
    stages = [range(0, group - 1), range(group - 1, 2 * group - 1), range(2 * group - 1, 3 * group - 1)]

    def device(peer):
        return {"dp": lax.bitwise_xor(own_dp, peer[0]), "expert": lax.bitwise_xor(own_expert, peer[1])}

    def there(p):
        start, rows, peer = pieces[p]
        return pltpu.make_async_remote_copy(
            src_ref=grouped.at[pl.ds(start, rows)], dst_ref=arrived.at[pl.ds(start, rows)],
            send_sem=there_send.at[p], recv_sem=there_recv.at[p], device_id=device(peer), device_id_type=mesh_id,
        )

    def down_columns(n):
        return pl.ds(pl.multiple_of(n * down_width, down_width), down_width)

    def back(n, p):
        start, rows, peer = pieces[p]
        return pltpu.make_async_remote_copy(
            src_ref=arrived.at[pl.ds(start, rows), down_columns(n)],
            dst_ref=returned.at[pl.ds(start, rows), down_columns(n)],
            send_sem=back_send.at[n, p], recv_sem=back_recv.at[n, p], device_id=device(peer), device_id_type=mesh_id,
        )

    def cache_copy(c):
        return pltpu.make_async_remote_copy(
            src_ref=leaving.at[c], dst_ref=coming.at[c], send_sem=cache_send.at[c], recv_sem=cache_recv.at[c],
            device_id={"dp": lax.bitwise_xor(own_dp, 1)}, device_id_type=mesh_id,
        )

    def delta_copy(n):
        return pltpu.make_async_remote_copy(
            src_ref=second.at[:, down_columns(n)], dst_ref=received.at[:, down_columns(n)],
            send_sem=delta_send.at[n], recv_sem=delta_recv.at[n],
            device_id={"section": lax.rem(own_section + 1, section_count)}, device_id_type=mesh_id,
        )

    def up_copy(f):
        columns = pl.ds(pl.multiple_of(f * up_width, up_width), up_width)
        return pltpu.make_async_copy(w_up.at[:, columns], up_buf.at[f], up_sem.at[f])

    def down_copy(n):
        return pltpu.make_async_copy(w_down.at[:, down_columns(n)], down_buf.at[n], down_sem.at[n])

    load_inputs = pltpu.make_async_copy(inputs, first, load_sem.at[0])
    load_out = pltpu.make_async_copy(out_cache, second, load_sem.at[1])
    load_in = pltpu.make_async_copy(in_cache, first, load_sem.at[2])
    store_out = pltpu.make_async_copy(second, out_moved, store_sem.at[0])
    store_in = pltpu.make_async_copy(first, in_moved, store_sem.at[1])

    load_inputs.start()
    load_out.start()

    @pl.loop(0, ups)
    def _(f):
        up_copy(f).start()

    barrier = pltpu.get_barrier_semaphore()
    for peer in near[1:] + far:
        pl.semaphore_signal(barrier, inc=1, device_id=device(peer), device_id_type=mesh_id)
    for by in (1, section_count - 1):
        pl.semaphore_signal(
            barrier, inc=1, device_id={"section": lax.rem(own_section + by, section_count)}, device_id_type=mesh_id
        )

    places = token_slots(routing, own_dp, own_expert, expert_count, dp_count, per_expert)
    numbers = rows_iota(slots, tok_rows, 0)
    select = one_hot((numbers == places[0]) | (numbers == places[1]))
    load_inputs.wait()
    for n in range(downs):
        columns = pl.ds(n * down_width, down_width)
        rows = jnp.dot(select, first[:, columns], preferred_element_type=jnp.float32).astype(jnp.bfloat16)
        grouped[:, columns] = rows
        arrived[:per_expert, columns] = rows[:per_expert]
    load_in.start()

    @pl.loop(0, downs)
    def _(n):
        down_copy(n).start()

    pl.semaphore_wait(barrier, len(near) + len(far) + 1)
    for p in range(len(pieces)):
        there(p).start()

    weights = gates[...].astype(jnp.float32)
    weights = weights / jnp.sum(weights, axis=0, keepdims=True)
    mixed = jnp.zeros((slots, tok_rows), jnp.float32)
    for k in range(TOPK):
        mixed = mixed + jnp.where(numbers == places[k], weights[k : k + 1, :], 0.0)
    mixed = mixed.T
    high = mixed.astype(jnp.bfloat16)
    mix[:tok_rows] = high
    mix[tok_rows:] = (mixed - high.astype(jnp.float32)).astype(jnp.bfloat16)

    other = lax.bitwise_xor(own_dp, 1)
    old_rows, leave_slots = sample_rows(sample_map, me, tok_rows, expert_count, other)
    send_pick = one_hot(rows_iota(moved_rows, tok_rows, 0) == leave_slots)
    their_rows, come_slots = sample_rows(
        sample_map, other * expert_count + own_expert, tok_rows, expert_count, own_dp
    )
    new_row, old_row = rows_iota(tok_rows, tok_rows, 0), rows_iota(tok_rows, tok_rows, 1)
    same_row = lax.rem(new_row, ROWS) == lax.rem(old_row, ROWS)
    new_sample = me * SAMP_DEV + lax.div(new_row, ROWS)
    own_pick[...] = one_hot(same_row & (new_sample == old_rows))
    far_pick[...] = lax.dot_general(
        one_hot(same_row & (new_sample == their_rows)),
        one_hot(rows_iota(moved_rows, tok_rows, 0) == come_slots),
        (((1,), (1,)), ((), ())),
        preferred_element_type=jnp.float32,
    ).astype(jnp.bfloat16)

    def send_cache(c, held):
        for n in range(downs):
            columns = pl.ds(n * down_width, down_width)
            leaving[c, :, columns] = jnp.dot(
                send_pick, held[:, columns], preferred_element_type=jnp.float32
            ).astype(jnp.bfloat16)
        cache_copy(c).start()

    load_out.wait()
    send_cache(0, second)

    def up_pass(start, fresh):
        @pl.loop(0, ups)
        def _(f):
            if fresh:
                up_copy(f).wait()
            value = jnp.dot(arrived[pl.ds(start, near_rows)], up_buf[f], preferred_element_type=jnp.float32)
            columns = pl.ds(pl.multiple_of(f * up_width, up_width), up_width)
            hidden[:, columns] = (0.5 * value * (1.0 + jnp.tanh(0.5 * value))).astype(jnp.bfloat16)

    def down_pass(start, stage, fresh):
        skip = per_expert if fresh else near_rows - chunk_rows

        @pl.loop(0, downs)
        def _(n):
            if fresh:
                down_copy(n).wait()
            value = jnp.dot(hidden[...], down_buf[n], preferred_element_type=jnp.float32).astype(jnp.bfloat16)
            if fresh:
                returned[:skip, down_columns(n)] = value[:skip]
            arrived[pl.ds(start + skip, near_rows - skip), down_columns(n)] = value[skip:]
            for p in stages[stage]:
                back(n, p).start()

    for p in stages[0]:
        there(p).wait_recv()
    up_pass(0, True)
    load_in.wait()
    send_cache(1, first)
    down_pass(0, 0, True)
    for c in range(2):
        for p in stages[1 + c]:
            there(p).wait_recv()
        up_pass(near_rows + (c - 1) * chunk_rows, False)
        down_pass(near_rows + (c - 1) * chunk_rows, 1 + c, False)

    for p in range(len(pieces)):
        there(p).wait_send()

    for c, held in enumerate((second, first)):
        cache_copy(c).wait()

        @pl.loop(0, downs)
        def _(n):
            columns = down_columns(n)
            total = jnp.dot(own_pick[...], held[:, columns], preferred_element_type=jnp.float32)
            total = total + jnp.dot(far_pick[...], coming[c, :, columns], preferred_element_type=jnp.float32)
            held[:, columns] = total.astype(jnp.bfloat16)

        (store_out, store_in)[c].start()

    @pl.when(own_section == 0)
    def _():
        grouped[:tok_rows] = jnp.zeros((tok_rows, width), jnp.bfloat16)
        blank = pltpu.make_async_copy(grouped.at[pl.ds(0, tok_rows)], received, store_sem.at[2])
        blank.start()
        blank.wait()

    store_out.wait()

    @pl.loop(0, downs)
    def _(n):
        columns = down_columns(n)
        for p in range(len(pieces)):
            back(n, p).wait_recv()
        both = jnp.dot(mix[...], returned[:, columns], preferred_element_type=jnp.float32)
        row = rows_iota(tok_rows, down_width, 0)
        sample, live = lax.div(row, ROWS), jnp.zeros_like(row)
        for j in range(SAMP_DEV):
            live = jnp.where(sample == j, lengths[j], live)
        change = both[:tok_rows] + both[tok_rows:] - second[:, columns].astype(jnp.float32)
        change = jnp.where(lax.rem(row, ROWS) < live, change, 0.0)
        second[:, columns] = change.astype(jnp.bfloat16)

        @pl.when(own_section < section_count - 1)
        def _():
            delta_copy(n).start()

        pltpu.make_async_copy(second.at[:, columns], delta.at[:, columns], delta_store.at[n]).start()

    store_in.wait()

    @pl.loop(0, downs)
    def _(n):
        columns = down_columns(n)
        pltpu.make_async_copy(second.at[:, columns], delta.at[:, columns], delta_store.at[n]).wait()
        for p in range(len(pieces)):
            back(n, p).wait_send()

        @pl.when(own_section < section_count - 1)
        def _():
            delta_copy(n).wait_send()

        @pl.when(own_section > 0)
        def _():
            delta_copy(n).wait_recv()


def run_section_kernel(routing, gates, lengths, sample_map, inputs, in_cache, out_cache, w_up, w_down, per_expert):
    dp_count, expert_count = lax.axis_size("dp"), lax.axis_size("expert")
    section_count = lax.axis_size("section")
    tok_rows, width = in_cache.shape
    slots, units = tok_rows * TOPK, w_up.shape[1]
    near_rows = slots // 2
    moved_rows = tok_rows // dp_count
    count = 3 * (dp_count * expert_count // 2) - 1
    vmem, smem = pl.BlockSpec(memory_space=pltpu.VMEM), pl.BlockSpec(memory_space=pltpu.SMEM)
    anywhere = pl.BlockSpec(memory_space=pl.ANY)
    dma = pltpu.SemaphoreType.DMA
    rows = jax.ShapeDtypeStruct((tok_rows, width), jnp.bfloat16)
    return pl.pallas_call(
        functools.partial(section_kernel, dp_count, expert_count, section_count, per_expert),
        out_shape=(rows, rows, rows, rows),
        in_specs=[vmem, vmem, smem, smem] + [anywhere] * 5,
        out_specs=(anywhere,) * 4,
        scratch_shapes=[
            pltpu.VMEM((UP_BLOCKS, width, units // UP_BLOCKS), jnp.bfloat16),
            pltpu.VMEM((DOWN_BLOCKS, units, width // DOWN_BLOCKS), jnp.bfloat16),
            pltpu.VMEM((tok_rows, width), jnp.bfloat16),
            pltpu.VMEM((tok_rows, width), jnp.bfloat16),
            pltpu.VMEM((2, moved_rows, width), jnp.bfloat16),
            pltpu.VMEM((2, moved_rows, width), jnp.bfloat16),
            pltpu.VMEM((slots, width), jnp.bfloat16),
            pltpu.VMEM((slots, width), jnp.bfloat16),
            pltpu.VMEM((near_rows, units), jnp.bfloat16),
            pltpu.VMEM((slots, width), jnp.bfloat16),
            pltpu.VMEM((2 * tok_rows, slots), jnp.bfloat16),
            pltpu.VMEM((tok_rows, tok_rows), jnp.bfloat16),
            pltpu.VMEM((tok_rows, moved_rows), jnp.bfloat16),
            dma((UP_BLOCKS,)),
            dma((DOWN_BLOCKS,)),
            dma((3,)),
            dma((count,)),
            dma((count,)),
            dma((DOWN_BLOCKS, count)),
            dma((DOWN_BLOCKS, count)),
            dma((2,)),
            dma((2,)),
            dma((3,)),
            dma((DOWN_BLOCKS,)),
            dma((DOWN_BLOCKS,)),
            dma((DOWN_BLOCKS,)),
        ],
        compiler_params=pltpu.CompilerParams(
            collective_id=0, has_side_effects=True, vmem_limit_bytes=KERNEL_VMEM
        ),
        cost_estimate=pl.CostEstimate(
            flops=4 * slots * width * units, bytes_accessed=4 * width * units, transcendentals=slots * units
        ),
    )(routing, gates, lengths, sample_map, inputs, in_cache, out_cache, w_up, w_down)


def fits_kernel(tok_rows, width, units, dp_count, expert_count):
    slots = tok_rows * TOPK
    halves = expert_count % 2 == 0 and expert_count & (expert_count - 1) == 0
    whole = units % (UP_BLOCKS * 128) == 0 and width % (DOWN_BLOCKS * 128) == 0
    rows = slots % (EXPERTS * 32) == 0 and tok_rows % 128 == 0
    needed = 2 * (2 * width * units + slots // 2 * (units + units // UP_BLOCKS) + 5 * slots * width)
    return dp_count == 2 and dp_count * expert_count == EXPERTS and halves and whole and rows and needed < KERNEL_VMEM


def per_device(inputs, in_cache, out_cache, w_up, w_down, routing, gate_table, lengths, sample_map):
    tok_rows, width = inputs.shape[1:]
    dp_count = lax.axis_size("dp")
    expert_count = lax.axis_size("expert")
    group_size = dp_count * expert_count
    slice_count = group_size // EXPERTS
    own_dp = lax.axis_index("dp")
    own_device = own_dp * expert_count + lax.axis_index("expert")
    cap_slots = max(1, SAMP_DEV // dp_count)
    per_expert = tok_rows * TOPK // EXPERTS

    if fits_kernel(tok_rows, width, w_up.shape[2], dp_count, expert_count):
        out_moved, delta_rows, in_moved, received = run_section_kernel(
            routing[0].T, gate_table[0].T, lengths, sample_map,
            inputs[0], in_cache[0], out_cache[0], w_up[0], w_down[0], per_expert,
        )
    else:
        select, mix = token_plan(routing[0], gate_table[0], per_expert)
        grouped = jnp.dot(select, inputs[0], preferred_element_type=jnp.float32).astype(jnp.bfloat16)
        grouped = grouped.reshape(EXPERTS, 1, per_expert, width)
        outgoing = jnp.broadcast_to(grouped, (EXPERTS, slice_count, per_expert, width)).reshape(
            group_size, per_expert, width
        )
        arrived = lax.all_to_all(outgoing, ("dp", "expert"), split_axis=0, concat_axis=0, tiled=True)

        to_send, arrival = cache_plan(sample_map, own_device, own_dp, dp_count, expert_count, cap_slots)
        send = jnp.concatenate(
            [
                in_cache[0].reshape(SAMP_DEV, 1, ROWS, width)[to_send],
                out_cache[0].reshape(SAMP_DEV, 1, ROWS, width)[to_send],
            ],
            axis=1,
        )
        send, arrived = lax.optimization_barrier((send, arrived))
        got = lax.all_to_all(send, "dp", split_axis=0, concat_axis=0, tiled=True)

        hidden = jax.nn.silu(
            jnp.dot(arrived.reshape(-1, width), w_up[0], preferred_element_type=jnp.float32)
        ).astype(jnp.bfloat16)
        partial_value = jnp.dot(hidden, w_down[0], preferred_element_type=jnp.float32).astype(jnp.bfloat16)
        returned = lax.all_to_all(
            partial_value.reshape(arrived.shape), ("dp", "expert"), split_axis=0, concat_axis=0, tiled=True
        ).reshape(-1, width)

        mix = jnp.broadcast_to(
            mix.reshape(tok_rows, EXPERTS, 1, per_expert), (tok_rows, EXPERTS, slice_count, per_expert)
        ).reshape(tok_rows, -1)
        high = mix.astype(jnp.bfloat16)
        low = (mix - high.astype(jnp.float32)).astype(jnp.bfloat16)
        both = jnp.dot(jnp.concatenate([high, low], axis=0), returned, preferred_element_type=jnp.float32)
        mixed = both[:tok_rows] + both[tok_rows:]

        in_moved = got[arrival, 0].reshape(tok_rows, width)
        out_moved = got[arrival, 1].reshape(tok_rows, width)

        row_numbers = jnp.arange(tok_rows, dtype=jnp.int32) % ROWS
        valid_rows = row_numbers < jnp.repeat(lengths, ROWS)
        delta_rows = jnp.where(
            valid_rows[:, None],
            (mixed - out_moved.astype(jnp.float32)).astype(jnp.bfloat16),
            jnp.zeros((), jnp.bfloat16),
        )
        received = from_behind(delta_rows, "section", 1)

    new_out = (out_moved.astype(jnp.float32) + delta_rows.astype(jnp.float32)).astype(jnp.bfloat16)
    next_input = (in_moved.astype(jnp.float32) + received.astype(jnp.float32)).astype(jnp.bfloat16)
    return (next_input[None], new_out[None])


def solution(mesh):
    split = P("section", ("dp", "expert"), None)
    placed = (split, split, split, P("section", None, ("dp", "expert")), split, split, split, P(("dp", "expert")), P())
    return jax.shard_map(per_device, mesh=mesh, in_specs=placed, out_specs=(split, split), check_vma=False)
```

```python
import functools

import jax
import jax.numpy as jnp
from jax import lax
from jax.experimental import pallas as pl
from jax.experimental.pallas import tpu as pltpu
from jax.sharding import PartitionSpec as P

EXPERTS = 8
TOPK = 2
ROWS = 16
SAMP_DEV = 8


def from_behind(value, axis, by):
    peers = lax.axis_size(axis)
    pairs = [(i, i + by) for i in range(peers) if 0 <= i + by < peers]
    return lax.ppermute(value, axis, pairs)


def cache_plan(sample_map, own_device, own_dp, dp_count, expert_count, cap_slots):
    total = sample_map.shape[0]
    ids = jnp.arange(total, dtype=jnp.int32)
    local = jnp.arange(SAMP_DEV, dtype=jnp.int32)
    own_map = lax.dynamic_slice_in_dim(sample_map, own_device * SAMP_DEV, SAMP_DEV)
    dest_dp = own_map // (SAMP_DEV * expert_count)
    slot = jnp.sum(
        ((dest_dp[:, None] == dest_dp[None, :]) & (local[None, :] < local[:, None])).astype(jnp.int32),
        axis=1,
    )
    places = jnp.arange(dp_count * cap_slots, dtype=jnp.int32)
    to_send = jnp.sum(
        jnp.where(places[:, None] == (dest_dp * cap_slots + slot)[None, :], local[None, :], 0), axis=1
    )
    wanted = own_device * SAMP_DEV + local
    sources = jnp.sum(jnp.where(sample_map[None, :] == wanted[:, None], ids[None, :], 0), axis=1)
    source_device = sources // SAMP_DEV
    earlier = (
        (ids[None, :] // SAMP_DEV == source_device[:, None])
        & (ids[None, :] < sources[:, None])
        & (sample_map[None, :] // (SAMP_DEV * expert_count) == own_dp)
    )
    arrival = source_device // expert_count * cap_slots + jnp.sum(earlier.astype(jnp.int32), axis=1)
    return to_send, arrival


def token_plan(routing, gate_table, per_expert):
    tok_rows = routing.shape[0]
    before = jnp.arange(tok_rows)[None, :] < jnp.arange(tok_rows)[:, None]
    weights = gate_table.astype(jnp.float32)
    weights = weights / jnp.sum(weights, axis=1, keepdims=True)
    slots = jnp.arange(EXPERTS * per_expert, dtype=jnp.int32)
    select, mix = 0, 0
    for k in range(TOPK):
        own = routing[:, k]
        rank = 0
        for j in range(TOPK):
            rank = rank + jnp.sum((before & (routing[:, j][None, :] == own[:, None])).astype(jnp.int32), axis=1)
        slot = own * per_expert + rank
        select = select + (slots[:, None] == slot[None, :]).astype(jnp.bfloat16)
        mix = mix + jnp.where(slots[None, :] == slot[:, None], weights[:, k][:, None], 0.0)
    return select, mix


UP_BLOCKS = 4
DOWN_BLOCKS = 4
CHUNKS = 2
FINISH_BLOCKS = 4
KERNEL_VMEM = 67043328


def iota(rows, columns, axis):
    return lax.broadcasted_iota(jnp.int32, (rows, columns), axis)


def one_hot(mask):
    return jnp.where(mask, 1.0, 0.0).astype(jnp.bfloat16)


def token_slots(routing, own_dp, own_expert, expert_count, per_expert):
    tok_rows = routing.shape[1]
    part_rows = per_expert // CHUNKS
    names = iota(16, tok_rows, 0)
    chosen = [routing[k : k + 1, :] for k in range(TOPK)]
    named = 0.0
    for own in chosen:
        named = named + jnp.where(names == own, 1.0, 0.0)
    before = one_hot(iota(tok_rows, tok_rows, 0) < iota(tok_rows, tok_rows, 1))
    ranks = jnp.dot(named.astype(jnp.bfloat16), before, preferred_element_type=jnp.float32)
    slots = []
    for own in chosen:
        rank = jnp.sum(jnp.where(names == own, ranks, 0.0), axis=0, keepdims=True).astype(jnp.int32)
        dd = lax.bitwise_xor(lax.div(own, expert_count), own_dp)
        m = lax.bitwise_xor(lax.rem(own, expert_count), own_expert)
        chunk = lax.div(rank, part_rows)
        slots.append(chunk * (EXPERTS * part_rows) + (dd * expert_count + m) * part_rows + lax.rem(rank, part_rows))
    return slots


def sample_rows(sample_map, device, tok_rows, expert_count, to_dp):
    lane = iota(1, tok_rows, 1)
    sample, within = lax.div(lane, ROWS), lax.rem(lane, ROWS)
    places, slots, used = jnp.zeros_like(lane), jnp.zeros_like(lane), 0
    for g in range(SAMP_DEV):
        place = sample_map[device * SAMP_DEV + g]
        goes = (lax.div(place, SAMP_DEV * expert_count) == to_dp).astype(jnp.int32)
        base = goes * (used * ROWS) - (1 - goes) * tok_rows
        places = jnp.where(sample == g, place, places)
        slots = jnp.where(sample == g, base, slots)
        used = used + goes
    return places, slots + within


def section_kernel(
    dp_count, expert_count, section_count, per_expert,
    routing_in, gates_in, lengths_in, sample_map_in, inputs, in_cache, out_cache, w_up, w_down,
    settled, in_moved, received,
    routing, gates, lengths, sample_map,
    up_buf, down_buf, first, second, leaving, coming, grouped, arrived, hidden, returned, mix, own_pick, far_pick,
    up_sem, down_sem, load_sem, there_send, there_recv, back_send, back_recv,
    cache_send, cache_recv, store_sem, settled_store, delta_send, delta_recv,
):
    own_dp, own_expert, own_section = lax.axis_index("dp"), lax.axis_index("expert"), lax.axis_index("section")
    me = own_dp * expert_count + own_expert
    tok_rows, width = inputs.shape
    slots = tok_rows * TOPK
    ups, up_width = up_buf.shape[0], up_buf.shape[2]
    downs, down_width = down_buf.shape[0], down_buf.shape[2]
    part_rows, chunk_rows = per_expert // CHUNKS, slots // CHUNKS
    moved_rows = tok_rows // dp_count
    blank = grouped.at[pl.ds(slots - tok_rows, tok_rows)]
    mesh_id = pl.DeviceIdType.MESH

    peers = [(dd, m) for dd in range(dp_count) for m in range(expert_count)]
    others = sorted(range(1, len(peers)), key=lambda i: (-peers[i][1], peers[i][0]))

    def device(i):
        dd, m = peers[i]
        return {"dp": lax.bitwise_xor(own_dp, dd), "expert": lax.bitwise_xor(own_expert, m)}

    def there(c, i):
        rows = pl.ds(c * chunk_rows + i * part_rows, part_rows)
        return pltpu.make_async_remote_copy(
            src_ref=grouped.at[rows], dst_ref=arrived.at[rows],
            send_sem=there_send.at[c], recv_sem=there_recv.at[c], device_id=device(i), device_id_type=mesh_id,
        )

    def down_columns(n):
        return pl.ds(pl.multiple_of(n * down_width, down_width), down_width)

    def back(n, c, i):
        rows = pl.ds(c * chunk_rows + i * part_rows, part_rows)
        return pltpu.make_async_remote_copy(
            src_ref=arrived.at[rows, down_columns(n)], dst_ref=returned.at[rows, down_columns(n)],
            send_sem=back_send.at[n], recv_sem=back_recv.at[n],
            device_id=device(i), device_id_type=mesh_id,
        )

    def all_there(c):
        rows = pl.ds(c * chunk_rows + part_rows, chunk_rows - part_rows)
        return pltpu.make_async_remote_copy(
            src_ref=grouped.at[rows], dst_ref=arrived.at[rows], send_sem=there_send.at[c], recv_sem=there_recv.at[c],
            device_id=device(others[0]), device_id_type=mesh_id,
        )

    def all_back(n):
        rows = pl.ds(0, slots - CHUNKS * part_rows)
        return pltpu.make_async_remote_copy(
            src_ref=arrived.at[rows, down_columns(n)], dst_ref=returned.at[rows, down_columns(n)],
            send_sem=back_send.at[n], recv_sem=back_recv.at[n], device_id=device(others[0]), device_id_type=mesh_id,
        )

    def cache_copy(c):
        rows = pl.ds(c * moved_rows, moved_rows)
        return pltpu.make_async_remote_copy(
            src_ref=leaving.at[rows], dst_ref=coming.at[rows], send_sem=cache_send.at[c], recv_sem=cache_recv.at[c],
            device_id={"dp": lax.bitwise_xor(own_dp, 1)}, device_id_type=mesh_id,
        )

    def delta_copy(n):
        return pltpu.make_async_remote_copy(
            src_ref=leaving.at[:, down_columns(n)], dst_ref=received.at[:, down_columns(n)],
            send_sem=delta_send.at[n], recv_sem=delta_recv.at[n],
            device_id={"section": lax.rem(own_section + 1, section_count)}, device_id_type=mesh_id,
        )

    def settled_out(n):
        columns = down_columns(n)
        return pltpu.make_async_copy(second.at[:, columns], settled.at[:, columns], settled_store.at[n])

    def up_copy(f):
        columns = pl.ds(pl.multiple_of(f * up_width, up_width), up_width)
        return pltpu.make_async_copy(w_up.at[:, columns], up_buf.at[f], up_sem.at[f])

    def down_copy(n):
        return pltpu.make_async_copy(w_down.at[:, down_columns(n)], down_buf.at[n], down_sem.at[n])

    small = ((routing_in, routing), (gates_in, gates), (lengths_in, lengths), (sample_map_in, sample_map))
    small = [pltpu.make_async_copy(source, held, load_sem.at[3 + i]) for i, (source, held) in enumerate(small)]
    load_inputs = pltpu.make_async_copy(inputs, first, load_sem.at[0])
    load_out = pltpu.make_async_copy(out_cache, second, load_sem.at[1])
    load_in = pltpu.make_async_copy(in_cache, first, load_sem.at[2])
    store_in = pltpu.make_async_copy(first, in_moved, store_sem.at[0])
    store_blank = pltpu.make_async_copy(blank, received, store_sem.at[1])

    small[0].start()
    load_inputs.start()
    for copy in small[1:]:
        copy.start()

    barrier = pltpu.get_barrier_semaphore()
    for i in others:
        pl.semaphore_signal(barrier, inc=1, device_id=device(i), device_id_type=mesh_id)
    for by in (1, section_count - 1):
        pl.semaphore_signal(
            barrier, inc=1, device_id={"section": lax.rem(own_section + by, section_count)}, device_id_type=mesh_id
        )

    load_out.start()

    @pl.loop(0, ups)
    def _(f):
        up_copy(f).start()

    with jax.named_scope("plan"):
        small[0].wait()
        places = token_slots(routing, own_dp, own_expert, expert_count, per_expert)
        numbers = iota(slots, tok_rows, 0)
        select = one_hot((numbers == places[0]) | (numbers == places[1]))

    def pack(c):
        for n in range(downs):
            columns = pl.ds(n * down_width, down_width)
            rows = jnp.dot(
                select[c * chunk_rows : (c + 1) * chunk_rows], first[:, columns], preferred_element_type=jnp.float32
            ).astype(jnp.bfloat16)
            grouped[c * chunk_rows : (c + 1) * chunk_rows, columns] = rows
            arrived[c * chunk_rows : c * chunk_rows + part_rows, columns] = rows[:part_rows]

    with jax.named_scope("pack"):
        load_inputs.wait()
        pack(0)

    with jax.named_scope("meet"):
        pl.semaphore_wait(barrier, len(others) + 2)
    for i in others:
        there(0, i).start()
    with jax.named_scope("packed"):
        pack(1)
    load_in.start()

    @pl.loop(0, downs)
    def _(n):
        down_copy(n).start()

    with jax.named_scope("picks"):
        for copy in small[1:]:
            copy.wait()
        weights = gates[...].astype(jnp.float32)
        weights = weights / jnp.sum(weights, axis=0, keepdims=True)
        mixed = jnp.zeros((slots, tok_rows), jnp.float32)
        for k in range(TOPK):
            mixed = mixed + jnp.where(numbers == places[k], weights[k : k + 1, :], 0.0)
        mixed = mixed.T
        high = mixed.astype(jnp.bfloat16)
        mix[:tok_rows] = high
        mix[tok_rows:] = (mixed - high.astype(jnp.float32)).astype(jnp.bfloat16)

        other = lax.bitwise_xor(own_dp, 1)
        partner = other * expert_count + own_expert
        old_rows, leave_slots = sample_rows(sample_map, me, tok_rows, expert_count, other)
        send_pick = one_hot(iota(moved_rows, tok_rows, 0) == leave_slots)
        their_rows, come_slots = sample_rows(sample_map, partner, tok_rows, expert_count, own_dp)
        new_row, old_row = iota(tok_rows, tok_rows, 0), iota(tok_rows, tok_rows, 1)
        same_row = lax.rem(new_row, ROWS) == lax.rem(old_row, ROWS)
        new_sample = me * SAMP_DEV + lax.div(new_row, ROWS)
        own_pick[...] = one_hot(same_row & (new_sample == old_rows))
        far_pick[...] = lax.dot_general(
            one_hot(same_row & (new_sample == their_rows)),
            one_hot(iota(moved_rows, tok_rows, 0) == come_slots),
            (((1,), (1,)), ((), ())),
            preferred_element_type=jnp.float32,
        ).astype(jnp.bfloat16)

    def send_cache(c, held):
        for n in range(downs):
            columns = pl.ds(n * down_width, down_width)
            leaving[c * moved_rows : (c + 1) * moved_rows, columns] = jnp.dot(
                send_pick, held[:, columns], preferred_element_type=jnp.float32
            ).astype(jnp.bfloat16)
        cache_copy(c).start()

    def up_pass(c):
        @pl.loop(0, ups)
        def _(f):
            if c == 0:
                up_copy(f).wait()
            rows = arrived[c * chunk_rows : (c + 1) * chunk_rows]
            value = jnp.dot(rows, up_buf[f], preferred_element_type=jnp.float32)
            columns = pl.ds(pl.multiple_of(f * up_width, up_width), up_width)
            hidden[:, columns] = (0.5 * value * (1.0 + jnp.tanh(0.5 * value))).astype(jnp.bfloat16)

    def down_pass(c):
        @pl.loop(0, downs)
        def _(n):
            if c == 0:
                down_copy(n).wait()
            value = jnp.dot(hidden[...], down_buf[n], preferred_element_type=jnp.float32).astype(jnp.bfloat16)
            returned[c * chunk_rows : c * chunk_rows + part_rows, down_columns(n)] = value[:part_rows]
            arrived[c * chunk_rows + part_rows : (c + 1) * chunk_rows, down_columns(n)] = value[part_rows:]
            for i in others:
                back(n, c, i).start()

    load_out.wait()
    send_cache(0, second)
    inner = (own_expert == expert_count // 2) | (own_expert == expert_count // 2 - 1)

    @pl.when(inner)
    def _():
        with jax.named_scope("sent"):
            all_there(0).wait_send()
        for i in others:
            there(1, i).start()

    with jax.named_scope("wait"):
        all_there(0).wait_recv()

    @pl.when(jnp.logical_not(inner))
    def _():
        for i in others:
            there(1, i).start()
        all_there(0).wait_send()

    load_in.wait()
    send_cache(1, first)
    for c in range(CHUNKS):
        if c > 0:
            with jax.named_scope("wait"):
                all_there(c).wait_recv()
        with jax.named_scope("up"):
            up_pass(c)
        with jax.named_scope("down"):
            down_pass(c)

    with jax.named_scope("moves"):
        all_there(1).wait_send()
        for c, held in enumerate((second, first)):
            with jax.named_scope("cache_wait"):
                cache_copy(c).wait()

            @pl.loop(0, downs)
            def _(n):
                columns = down_columns(n)
                come = coming[c * moved_rows : (c + 1) * moved_rows, columns]
                total = jnp.dot(own_pick[...], held[:, columns], preferred_element_type=jnp.float32)
                total = total + jnp.dot(far_pick[...], come, preferred_element_type=jnp.float32)
                held[:, columns] = total.astype(jnp.bfloat16)

        store_in.start()

    @pl.when(own_section == 0)
    def _():
        blank[...] = jnp.zeros((tok_rows, width), jnp.bfloat16)
        store_blank.start()

    @pl.loop(0, downs)
    def _(n):
        columns = down_columns(n)
        with jax.named_scope("back_wait"):
            all_back(n).wait_recv()
        both = jnp.dot(mix[...], returned[:, columns], preferred_element_type=jnp.float32)
        row = iota(tok_rows, down_width, 0)
        sample, live = lax.div(row, ROWS), jnp.zeros_like(row)
        for j in range(SAMP_DEV):
            live = jnp.where(sample == j, lengths[j], live)
        old = second[:, columns].astype(jnp.float32)
        change = jnp.where(lax.rem(row, ROWS) < live, both[:tok_rows] + both[tok_rows:] - old, 0.0)
        change = change.astype(jnp.bfloat16)
        leaving[:, columns] = change

        @pl.when(own_section < section_count - 1)
        def _():
            delta_copy(n).start()

        second[:, columns] = (old + change.astype(jnp.float32)).astype(jnp.bfloat16)
        settled_out(n).start()

    store_in.wait()

    @pl.when(own_section == 0)
    def _():
        store_blank.wait()

    @pl.loop(0, downs)
    def _(n):
        all_back(n).wait_send()
        settled_out(n).wait()

        @pl.when(own_section < section_count - 1)
        def _():
            delta_copy(n).wait_send()

        @pl.when(own_section > 0)
        def _():
            with jax.named_scope("delta_wait"):
                delta_copy(n).wait_recv()


def run_section_kernel(routing, gates, lengths, sample_map, inputs, in_cache, out_cache, w_up, w_down, per_expert):
    dp_count, expert_count = lax.axis_size("dp"), lax.axis_size("expert")
    section_count = lax.axis_size("section")
    tok_rows, width = in_cache.shape
    slots, units = tok_rows * TOPK, w_up.shape[1]
    moved_rows = tok_rows // dp_count
    anywhere = pl.BlockSpec(memory_space=pl.ANY)
    dma = pltpu.SemaphoreType.DMA
    rows = jax.ShapeDtypeStruct((tok_rows, width), jnp.bfloat16)
    return pl.pallas_call(
        functools.partial(section_kernel, dp_count, expert_count, section_count, per_expert),
        out_shape=(rows, rows, rows),
        in_specs=[anywhere] * 9,
        out_specs=(anywhere,) * 3,
        scratch_shapes=[
            pltpu.VMEM(routing.shape, jnp.int32),
            pltpu.VMEM(gates.shape, jnp.int32),
            pltpu.SMEM(lengths.shape, jnp.int32),
            pltpu.SMEM(sample_map.shape, jnp.int32),
            pltpu.VMEM((UP_BLOCKS, width, units // UP_BLOCKS), jnp.bfloat16),
            pltpu.VMEM((DOWN_BLOCKS, units, width // DOWN_BLOCKS), jnp.bfloat16),
            pltpu.VMEM((tok_rows, width), jnp.bfloat16),
            pltpu.VMEM((tok_rows, width), jnp.bfloat16),
            pltpu.VMEM((2 * moved_rows, width), jnp.bfloat16),
            pltpu.VMEM((2 * moved_rows, width), jnp.bfloat16),
            pltpu.VMEM((slots, width), jnp.bfloat16),
            pltpu.VMEM((slots, width), jnp.bfloat16),
            pltpu.VMEM((slots // CHUNKS, units), jnp.bfloat16),
            pltpu.VMEM((slots, width), jnp.bfloat16),
            pltpu.VMEM((2 * tok_rows, slots), jnp.bfloat16),
            pltpu.VMEM((tok_rows, tok_rows), jnp.bfloat16),
            pltpu.VMEM((tok_rows, moved_rows), jnp.bfloat16),
            dma((UP_BLOCKS,)),
            dma((DOWN_BLOCKS,)),
            dma((7,)),
            dma((CHUNKS,)),
            dma((CHUNKS,)),
            dma((DOWN_BLOCKS,)),
            dma((DOWN_BLOCKS,)),
            dma((2,)),
            dma((2,)),
            dma((2,)),
            dma((DOWN_BLOCKS,)),
            dma((DOWN_BLOCKS,)),
            dma((DOWN_BLOCKS,)),
        ],
        compiler_params=pltpu.CompilerParams(
            collective_id=0, has_side_effects=True, vmem_limit_bytes=KERNEL_VMEM
        ),
        cost_estimate=pl.CostEstimate(
            flops=4 * slots * width * units, bytes_accessed=4 * width * units, transcendentals=slots * units
        ),
    )(routing, gates, lengths, sample_map, inputs, in_cache, out_cache, w_up, w_down)


def finish_kernel(settled, in_moved, received, next_input, new_out, old, base, change, load_sem, store_sem):
    blocks = load_sem.shape[1]
    block_rows = old.shape[0] // blocks

    def copy(source, target, sem, b):
        rows = pl.ds(b * block_rows, block_rows)
        return pltpu.make_async_copy(source.at[rows], target.at[rows], sem.at[b])

    loads = [(in_moved, base, load_sem.at[0]), (received, change, load_sem.at[1]), (settled, old, load_sem.at[2])]
    for b in range(blocks):
        for load in loads[:2]:
            copy(*load, b).start()
    for b in range(blocks):
        copy(*loads[2], b).start()
    for b in range(blocks):
        rows = pl.ds(b * block_rows, block_rows)
        for load in loads[:2]:
            copy(*load, b).wait()
        base[rows] = (base[rows].astype(jnp.float32) + change[rows].astype(jnp.float32)).astype(jnp.bfloat16)
        copy(base, next_input, store_sem.at[0], b).start()
    for b in range(blocks):
        copy(*loads[2], b).wait()
        copy(old, new_out, store_sem.at[1], b).start()
    for b in range(blocks):
        copy(base, next_input, store_sem.at[0], b).wait()
        copy(old, new_out, store_sem.at[1], b).wait()


def run_finish_kernel(settled, in_moved, received):
    rows = jax.ShapeDtypeStruct(settled.shape, settled.dtype)
    anywhere = pl.BlockSpec(memory_space=pl.ANY)
    return pl.pallas_call(
        finish_kernel,
        out_shape=(rows, rows),
        in_specs=[anywhere] * 3,
        out_specs=(anywhere,) * 2,
        scratch_shapes=[pltpu.VMEM(settled.shape, settled.dtype)] * 3
        + [pltpu.SemaphoreType.DMA((3, FINISH_BLOCKS)), pltpu.SemaphoreType.DMA((2, FINISH_BLOCKS))],
    )(settled, in_moved, received)


def fits_kernel(tok_rows, width, units, dp_count, expert_count):
    slots = tok_rows * TOPK
    powers = expert_count & (expert_count - 1) == 0
    whole = units % (UP_BLOCKS * 128) == 0 and width % (DOWN_BLOCKS * 128) == 0
    rows = slots % (EXPERTS * CHUNKS * 16) == 0 and tok_rows % 128 == 0
    needed = 2 * (2 * width * units + slots // 2 * (units + units // UP_BLOCKS) + 5 * slots * width)
    return dp_count == 2 and dp_count * expert_count == EXPERTS and powers and whole and rows and needed < KERNEL_VMEM


def per_device(inputs, in_cache, out_cache, w_up, w_down, routing, gate_table, lengths, sample_map):
    tok_rows, width = inputs.shape[1:]
    dp_count = lax.axis_size("dp")
    expert_count = lax.axis_size("expert")
    group_size = dp_count * expert_count
    slice_count = group_size // EXPERTS
    own_dp = lax.axis_index("dp")
    own_device = own_dp * expert_count + lax.axis_index("expert")
    cap_slots = max(1, SAMP_DEV // dp_count)
    per_expert = tok_rows * TOPK // EXPERTS

    if fits_kernel(tok_rows, width, w_up.shape[2], dp_count, expert_count):
        settled, in_moved, received = run_section_kernel(
            routing[0].T, gate_table[0].T, lengths, sample_map,
            inputs[0], in_cache[0], out_cache[0], w_up[0], w_down[0], per_expert,
        )
        next_input, new_out = run_finish_kernel(settled, in_moved, received)
    else:
        select, mix = token_plan(routing[0], gate_table[0], per_expert)
        grouped = jnp.dot(select, inputs[0], preferred_element_type=jnp.float32).astype(jnp.bfloat16)
        grouped = grouped.reshape(EXPERTS, 1, per_expert, width)
        outgoing = jnp.broadcast_to(grouped, (EXPERTS, slice_count, per_expert, width)).reshape(
            group_size, per_expert, width
        )
        arrived = lax.all_to_all(outgoing, ("dp", "expert"), split_axis=0, concat_axis=0, tiled=True)

        to_send, arrival = cache_plan(sample_map, own_device, own_dp, dp_count, expert_count, cap_slots)
        send = jnp.concatenate(
            [
                in_cache[0].reshape(SAMP_DEV, 1, ROWS, width)[to_send],
                out_cache[0].reshape(SAMP_DEV, 1, ROWS, width)[to_send],
            ],
            axis=1,
        )
        send, arrived = lax.optimization_barrier((send, arrived))
        got = lax.all_to_all(send, "dp", split_axis=0, concat_axis=0, tiled=True)

        hidden = jax.nn.silu(
            jnp.dot(arrived.reshape(-1, width), w_up[0], preferred_element_type=jnp.float32)
        ).astype(jnp.bfloat16)
        partial_value = jnp.dot(hidden, w_down[0], preferred_element_type=jnp.float32).astype(jnp.bfloat16)
        returned = lax.all_to_all(
            partial_value.reshape(arrived.shape), ("dp", "expert"), split_axis=0, concat_axis=0, tiled=True
        ).reshape(-1, width)

        mix = jnp.broadcast_to(
            mix.reshape(tok_rows, EXPERTS, 1, per_expert), (tok_rows, EXPERTS, slice_count, per_expert)
        ).reshape(tok_rows, -1)
        high = mix.astype(jnp.bfloat16)
        low = (mix - high.astype(jnp.float32)).astype(jnp.bfloat16)
        both = jnp.dot(jnp.concatenate([high, low], axis=0), returned, preferred_element_type=jnp.float32)
        mixed = both[:tok_rows] + both[tok_rows:]

        in_moved = got[arrival, 0].reshape(tok_rows, width)
        out_moved = got[arrival, 1].reshape(tok_rows, width)

        row_numbers = jnp.arange(tok_rows, dtype=jnp.int32) % ROWS
        valid_rows = row_numbers < jnp.repeat(lengths, ROWS)
        delta_rows = jnp.where(
            valid_rows[:, None],
            (mixed - out_moved.astype(jnp.float32)).astype(jnp.bfloat16),
            jnp.zeros((), jnp.bfloat16),
        )
        received = from_behind(delta_rows, "section", 1)
        new_out = (out_moved.astype(jnp.float32) + delta_rows.astype(jnp.float32)).astype(jnp.bfloat16)
        next_input = (in_moved.astype(jnp.float32) + received.astype(jnp.float32)).astype(jnp.bfloat16)
    return (next_input[None], new_out[None])


def solution(mesh):
    split = P("section", ("dp", "expert"), None)
    placed = (split, split, split, P("section", None, ("dp", "expert")), split, split, split, P(("dp", "expert")), P())
    return jax.shard_map(per_device, mesh=mesh, in_specs=placed, out_specs=(split, split), check_vma=False)
```

```python
import functools

import jax
import jax.numpy as jnp
from jax import lax
from jax.experimental import pallas as pl
from jax.experimental.pallas import tpu as pltpu
from jax.sharding import PartitionSpec as P

EXPERTS = 8
TOPK = 2
ROWS = 16
SAMP_DEV = 8


def from_behind(value, axis, by):
    peers = lax.axis_size(axis)
    pairs = [(i, i + by) for i in range(peers) if 0 <= i + by < peers]
    return lax.ppermute(value, axis, pairs)


def cache_plan(sample_map, own_device, own_dp, dp_count, expert_count, cap_slots):
    total = sample_map.shape[0]
    ids = jnp.arange(total, dtype=jnp.int32)
    local = jnp.arange(SAMP_DEV, dtype=jnp.int32)
    own_map = lax.dynamic_slice_in_dim(sample_map, own_device * SAMP_DEV, SAMP_DEV)
    dest_dp = own_map // (SAMP_DEV * expert_count)
    slot = jnp.sum(
        ((dest_dp[:, None] == dest_dp[None, :]) & (local[None, :] < local[:, None])).astype(jnp.int32),
        axis=1,
    )
    places = jnp.arange(dp_count * cap_slots, dtype=jnp.int32)
    to_send = jnp.sum(
        jnp.where(places[:, None] == (dest_dp * cap_slots + slot)[None, :], local[None, :], 0), axis=1
    )
    wanted = own_device * SAMP_DEV + local
    sources = jnp.sum(jnp.where(sample_map[None, :] == wanted[:, None], ids[None, :], 0), axis=1)
    source_device = sources // SAMP_DEV
    earlier = (
        (ids[None, :] // SAMP_DEV == source_device[:, None])
        & (ids[None, :] < sources[:, None])
        & (sample_map[None, :] // (SAMP_DEV * expert_count) == own_dp)
    )
    arrival = source_device // expert_count * cap_slots + jnp.sum(earlier.astype(jnp.int32), axis=1)
    return to_send, arrival


def token_plan(routing, gate_table, per_expert):
    tok_rows = routing.shape[0]
    before = jnp.arange(tok_rows)[None, :] < jnp.arange(tok_rows)[:, None]
    weights = gate_table.astype(jnp.float32)
    weights = weights / jnp.sum(weights, axis=1, keepdims=True)
    slots = jnp.arange(EXPERTS * per_expert, dtype=jnp.int32)
    select, mix = 0, 0
    for k in range(TOPK):
        own = routing[:, k]
        rank = 0
        for j in range(TOPK):
            rank = rank + jnp.sum((before & (routing[:, j][None, :] == own[:, None])).astype(jnp.int32), axis=1)
        slot = own * per_expert + rank
        select = select + (slots[:, None] == slot[None, :]).astype(jnp.bfloat16)
        mix = mix + jnp.where(slots[None, :] == slot[:, None], weights[:, k][:, None], 0.0)
    return select, mix


UP_BLOCKS = 4
DOWN_BLOCKS = 8
MIX_BLOCKS = 4
CHUNKS = 2
DOWN_SLOTS = 4
FINISH_BLOCKS = 4
DEVICE_VMEM = 67043328
KERNEL_VMEM = 52 * 1024 * 1024


def iota(rows, columns, axis):
    return lax.broadcasted_iota(jnp.int32, (rows, columns), axis)


def one_hot(mask):
    return jnp.where(mask, 1.0, 0.0).astype(jnp.bfloat16)


def token_slots(routing, own_dp, own_expert, expert_count, per_expert):
    tok_rows = routing.shape[1]
    part_rows = per_expert // CHUNKS
    names = iota(16, tok_rows, 0)
    chosen = [routing[k : k + 1, :] for k in range(TOPK)]
    named = 0.0
    for own in chosen:
        named = named + jnp.where(names == own, 1.0, 0.0)
    before = one_hot(iota(tok_rows, tok_rows, 0) < iota(tok_rows, tok_rows, 1))
    ranks = jnp.dot(named.astype(jnp.bfloat16), before, preferred_element_type=jnp.float32)
    slots = []
    for own in chosen:
        rank = jnp.sum(jnp.where(names == own, ranks, 0.0), axis=0, keepdims=True).astype(jnp.int32)
        dd = lax.bitwise_xor(lax.div(own, expert_count), own_dp)
        m = lax.bitwise_xor(lax.rem(own, expert_count), own_expert)
        chunk = lax.div(rank, part_rows)
        slots.append(chunk * (EXPERTS * part_rows) + (dd * expert_count + m) * part_rows + lax.rem(rank, part_rows))
    return slots


def sample_rows(sample_map, device, tok_rows, expert_count, to_dp):
    lane = iota(1, tok_rows, 1)
    sample, within = lax.div(lane, ROWS), lax.rem(lane, ROWS)
    places, slots, used = jnp.zeros_like(lane), jnp.zeros_like(lane), 0
    for g in range(SAMP_DEV):
        place = sample_map[device * SAMP_DEV + g]
        goes = (lax.div(place, SAMP_DEV * expert_count) == to_dp).astype(jnp.int32)
        base = goes * (used * ROWS) - (1 - goes) * tok_rows
        places = jnp.where(sample == g, place, places)
        slots = jnp.where(sample == g, base, slots)
        used = used + goes
    return places, slots + within


def section_kernel(
    dp_count, expert_count, section_count, per_expert,
    routing_in, gates_in, lengths_in, sample_map_in, inputs, in_cache, out_cache, w_up, w_down,
    second, first, received,
    routing, gates, lengths, sample_map,
    up_buf, down_buf, leaving, coming, grouped, arrived, hidden, returned, mix, own_pick, far_pick,
    up_sem, down_sem, load_sem, there_send, there_recv, back_send, back_recv,
    cache_send, cache_recv, delta_send, delta_recv,
):
    own_dp, own_expert, own_section = lax.axis_index("dp"), lax.axis_index("expert"), lax.axis_index("section")
    me = own_dp * expert_count + own_expert
    tok_rows, width = inputs.shape
    slots = tok_rows * TOPK
    ups, up_width = up_buf.shape[0], up_buf.shape[2]
    down_width = down_buf.shape[2]
    downs = width // down_width
    mixes, mix_width = MIX_BLOCKS, width // MIX_BLOCKS
    part_rows, chunk_rows = per_expert // CHUNKS, slots // CHUNKS
    moved_rows = tok_rows // dp_count
    mesh_id = pl.DeviceIdType.MESH

    peers = [(dd, m) for dd in range(dp_count) for m in range(expert_count)]
    others = sorted(range(1, len(peers)), key=lambda i: (-peers[i][1], peers[i][0]))

    def device(i):
        dd, m = peers[i]
        return {"dp": lax.bitwise_xor(own_dp, dd), "expert": lax.bitwise_xor(own_expert, m)}

    def there(c, i):
        rows = pl.ds(c * chunk_rows + i * part_rows, part_rows)
        return pltpu.make_async_remote_copy(
            src_ref=grouped.at[rows], dst_ref=arrived.at[rows],
            send_sem=there_send.at[c], recv_sem=there_recv.at[c], device_id=device(i), device_id_type=mesh_id,
        )

    def down_columns(n):
        return pl.ds(pl.multiple_of(n * down_width, down_width), down_width)

    def back(n, c, i):
        rows = pl.ds(c * chunk_rows + i * part_rows, part_rows)
        return pltpu.make_async_remote_copy(
            src_ref=arrived.at[rows, down_columns(n)], dst_ref=returned.at[rows, down_columns(n)],
            send_sem=back_send.at[n], recv_sem=back_recv.at[n],
            device_id=device(i), device_id_type=mesh_id,
        )

    def all_there(c):
        rows = pl.ds(c * chunk_rows + part_rows, chunk_rows - part_rows)
        return pltpu.make_async_remote_copy(
            src_ref=grouped.at[rows], dst_ref=arrived.at[rows], send_sem=there_send.at[c], recv_sem=there_recv.at[c],
            device_id=device(others[0]), device_id_type=mesh_id,
        )

    def all_back(n):
        rows = pl.ds(0, slots - CHUNKS * part_rows)
        return pltpu.make_async_remote_copy(
            src_ref=arrived.at[rows, down_columns(n)], dst_ref=returned.at[rows, down_columns(n)],
            send_sem=back_send.at[n], recv_sem=back_recv.at[n], device_id=device(others[0]), device_id_type=mesh_id,
        )

    def cache_copy(c):
        rows = pl.ds(c * moved_rows, moved_rows)
        return pltpu.make_async_remote_copy(
            src_ref=leaving.at[rows], dst_ref=coming.at[rows], send_sem=cache_send.at[c], recv_sem=cache_recv.at[c],
            device_id={"dp": lax.bitwise_xor(own_dp, 1)}, device_id_type=mesh_id,
        )

    def mix_columns(n):
        return pl.ds(pl.multiple_of(n * mix_width, mix_width), mix_width)

    def delta_copy(n):
        return pltpu.make_async_remote_copy(
            src_ref=leaving.at[:, mix_columns(n)], dst_ref=received.at[:, mix_columns(n)],
            send_sem=delta_send.at[n], recv_sem=delta_recv.at[n],
            device_id={"section": lax.rem(own_section + 1, section_count)}, device_id_type=mesh_id,
        )

    def up_copy(f):
        columns = pl.ds(pl.multiple_of(f * up_width, up_width), up_width)
        return pltpu.make_async_copy(w_up.at[:, columns], up_buf.at[f], up_sem.at[f])

    def down_copy(n):
        slot = lax.rem(n, DOWN_SLOTS)
        return pltpu.make_async_copy(w_down.at[:, down_columns(lax.rem(n, downs))], down_buf.at[slot], down_sem.at[slot])

    small = ((routing_in, routing), (gates_in, gates), (lengths_in, lengths), (sample_map_in, sample_map))
    small = [pltpu.make_async_copy(source, held, load_sem.at[3 + i]) for i, (source, held) in enumerate(small)]
    load_inputs = pltpu.make_async_copy(inputs, first, load_sem.at[0])
    load_out = pltpu.make_async_copy(out_cache, second, load_sem.at[1])
    load_in = pltpu.make_async_copy(in_cache, first, load_sem.at[2])

    small[0].start()
    load_inputs.start()
    for copy in small[1:]:
        copy.start()

    barrier = pltpu.get_barrier_semaphore()
    for i in others:
        pl.semaphore_signal(barrier, inc=1, device_id=device(i), device_id_type=mesh_id)
    for by in (1, section_count - 1):
        pl.semaphore_signal(
            barrier, inc=1, device_id={"section": lax.rem(own_section + by, section_count)}, device_id_type=mesh_id
        )

    load_out.start()

    @pl.loop(0, ups)
    def _(f):
        up_copy(f).start()

    with jax.named_scope("plan"):
        small[0].wait()
        places = token_slots(routing, own_dp, own_expert, expert_count, per_expert)
        numbers = iota(slots, tok_rows, 0)
        select = one_hot((numbers == places[0]) | (numbers == places[1]))

    def pack(c):
        for n in range(mixes):
            columns = pl.ds(n * mix_width, mix_width)
            rows = jnp.dot(
                select[c * chunk_rows : (c + 1) * chunk_rows], first[:, columns], preferred_element_type=jnp.float32
            ).astype(jnp.bfloat16)
            grouped[c * chunk_rows : (c + 1) * chunk_rows, columns] = rows
            arrived[c * chunk_rows : c * chunk_rows + part_rows, columns] = rows[:part_rows]

    with jax.named_scope("pack"):
        load_inputs.wait()
        pack(0)

    with jax.named_scope("meet"):
        pl.semaphore_wait(barrier, len(others) + 2)
    for i in others:
        there(0, i).start()
    with jax.named_scope("packed"):
        pack(1)
    load_in.start()

    for n in range(DOWN_SLOTS):
        down_copy(n).start()

    with jax.named_scope("picks"):
        for copy in small[1:]:
            copy.wait()
        weights = gates[...].astype(jnp.float32)
        weights = weights / jnp.sum(weights, axis=0, keepdims=True)
        mixed = jnp.zeros((slots, tok_rows), jnp.float32)
        for k in range(TOPK):
            mixed = mixed + jnp.where(numbers == places[k], weights[k : k + 1, :], 0.0)
        mixed = mixed.T
        high = mixed.astype(jnp.bfloat16)
        mix[:tok_rows] = high
        mix[tok_rows:] = (mixed - high.astype(jnp.float32)).astype(jnp.bfloat16)

        other = lax.bitwise_xor(own_dp, 1)
        partner = other * expert_count + own_expert
        old_rows, leave_slots = sample_rows(sample_map, me, tok_rows, expert_count, other)
        send_pick = one_hot(iota(moved_rows, tok_rows, 0) == leave_slots)
        their_rows, come_slots = sample_rows(sample_map, partner, tok_rows, expert_count, own_dp)
        new_row, old_row = iota(tok_rows, tok_rows, 0), iota(tok_rows, tok_rows, 1)
        same_row = lax.rem(new_row, ROWS) == lax.rem(old_row, ROWS)
        new_sample = me * SAMP_DEV + lax.div(new_row, ROWS)
        own_pick[...] = one_hot(same_row & (new_sample == old_rows))
        far_pick[...] = lax.dot_general(
            one_hot(same_row & (new_sample == their_rows)),
            one_hot(iota(moved_rows, tok_rows, 0) == come_slots),
            (((1,), (1,)), ((), ())),
            preferred_element_type=jnp.float32,
        ).astype(jnp.bfloat16)

    def send_cache(c, held):
        for n in range(mixes):
            columns = pl.ds(n * mix_width, mix_width)
            leaving[c * moved_rows : (c + 1) * moved_rows, columns] = jnp.dot(
                send_pick, held[:, columns], preferred_element_type=jnp.float32
            ).astype(jnp.bfloat16)
        cache_copy(c).start()

    def up_pass(c):
        @pl.loop(0, ups)
        def _(f):
            if c == 0:
                up_copy(f).wait()
            rows = arrived[c * chunk_rows : (c + 1) * chunk_rows]
            value = jnp.dot(rows, up_buf[f], preferred_element_type=jnp.float32)
            columns = pl.ds(pl.multiple_of(f * up_width, up_width), up_width)
            hidden[:, columns] = (0.5 * value * (1.0 + jnp.tanh(0.5 * value))).astype(jnp.bfloat16)

    def down_pass(c):
        @pl.loop(0, downs)
        def _(n):
            turn = c * downs + n
            down_copy(turn).wait()
            value = jnp.dot(
                hidden[...], down_buf[lax.rem(turn, DOWN_SLOTS)], preferred_element_type=jnp.float32
            ).astype(jnp.bfloat16)
            returned[c * chunk_rows : c * chunk_rows + part_rows, down_columns(n)] = value[:part_rows]
            arrived[c * chunk_rows + part_rows : (c + 1) * chunk_rows, down_columns(n)] = value[part_rows:]
            for i in others:
                back(n, c, i).start()

            @pl.when(turn + DOWN_SLOTS < CHUNKS * downs)
            def _():
                down_copy(turn + DOWN_SLOTS).start()

    load_out.wait()
    send_cache(0, second)
    inner = (own_expert == expert_count // 2) | (own_expert == expert_count // 2 - 1)

    @pl.when(inner)
    def _():
        with jax.named_scope("sent"):
            all_there(0).wait_send()
        for i in others:
            there(1, i).start()

    with jax.named_scope("wait"):
        all_there(0).wait_recv()

    @pl.when(jnp.logical_not(inner))
    def _():
        for i in others:
            there(1, i).start()
        all_there(0).wait_send()

    load_in.wait()
    send_cache(1, first)
    for c in range(CHUNKS):
        if c > 0:
            with jax.named_scope("wait"):
                all_there(c).wait_recv()
        with jax.named_scope("up"):
            up_pass(c)
        with jax.named_scope("down"):
            down_pass(c)

    with jax.named_scope("moves"):
        all_there(1).wait_send()
        for c, held in enumerate((second, first)):
            with jax.named_scope("cache_wait"):
                cache_copy(c).wait()

            @pl.loop(0, mixes)
            def _(n):
                columns = mix_columns(n)
                come = coming[c * moved_rows : (c + 1) * moved_rows, columns]
                total = jnp.dot(own_pick[...], held[:, columns], preferred_element_type=jnp.float32)
                total = total + jnp.dot(far_pick[...], come, preferred_element_type=jnp.float32)
                held[:, columns] = total.astype(jnp.bfloat16)


    @pl.when(own_section == 0)
    def _():
        received[...] = jnp.zeros((tok_rows, width), jnp.bfloat16)

    @pl.loop(0, mixes)
    def _(n):
        columns = mix_columns(n)
        with jax.named_scope("back_wait"):
            for b in range(downs // mixes):
                all_back(n * (downs // mixes) + b).wait_recv()
        both = jnp.dot(mix[...], returned[:, columns], preferred_element_type=jnp.float32)
        row = iota(tok_rows, mix_width, 0)
        sample, live = lax.div(row, ROWS), jnp.zeros_like(row)
        for j in range(SAMP_DEV):
            live = jnp.where(sample == j, lengths[j], live)
        old = second[:, columns].astype(jnp.float32)
        change = jnp.where(lax.rem(row, ROWS) < live, both[:tok_rows] + both[tok_rows:] - old, 0.0)
        change = change.astype(jnp.bfloat16)
        leaving[:, columns] = change

        @pl.when(own_section < section_count - 1)
        def _():
            delta_copy(n).start()

        second[:, columns] = (old + change.astype(jnp.float32)).astype(jnp.bfloat16)

    @pl.loop(0, downs)
    def _(n):
        all_back(n).wait_send()

    @pl.loop(0, mixes)
    def _(n):

        @pl.when(own_section < section_count - 1)
        def _():
            delta_copy(n).wait_send()

        @pl.when(own_section > 0)
        def _():
            with jax.named_scope("delta_wait"):
                delta_copy(n).wait_recv()


def run_section_kernel(routing, gates, lengths, sample_map, inputs, in_cache, out_cache, w_up, w_down, per_expert):
    dp_count, expert_count = lax.axis_size("dp"), lax.axis_size("expert")
    section_count = lax.axis_size("section")
    tok_rows, width = in_cache.shape
    slots, units = tok_rows * TOPK, w_up.shape[1]
    moved_rows = tok_rows // dp_count
    operands = (routing, gates, lengths, sample_map, inputs, in_cache, out_cache, w_up, w_down)
    operands = [pltpu.with_memory_space_constraint(operand, pltpu.HBM) for operand in operands]
    far_memory = pl.BlockSpec(memory_space=pltpu.HBM)
    dma = pltpu.SemaphoreType.DMA
    rows = jax.ShapeDtypeStruct((tok_rows, width), jnp.bfloat16)
    return pl.pallas_call(
        functools.partial(section_kernel, dp_count, expert_count, section_count, per_expert),
        out_shape=(rows, rows, rows),
        in_specs=[far_memory] * len(operands),
        out_specs=(pl.BlockSpec(memory_space=pltpu.VMEM),) * 3,
        scratch_shapes=[
            pltpu.VMEM(routing.shape, jnp.int32),
            pltpu.VMEM(gates.shape, jnp.int32),
            pltpu.SMEM(lengths.shape, jnp.int32),
            pltpu.SMEM(sample_map.shape, jnp.int32),
            pltpu.VMEM((UP_BLOCKS, width, units // UP_BLOCKS), jnp.bfloat16),
            pltpu.VMEM((DOWN_SLOTS, units, width // DOWN_BLOCKS), jnp.bfloat16),
            pltpu.VMEM((2 * moved_rows, width), jnp.bfloat16),
            pltpu.VMEM((2 * moved_rows, width), jnp.bfloat16),
            pltpu.VMEM((slots, width), jnp.bfloat16),
            pltpu.VMEM((slots, width), jnp.bfloat16),
            pltpu.VMEM((slots // CHUNKS, units), jnp.bfloat16),
            pltpu.VMEM((slots, width), jnp.bfloat16),
            pltpu.VMEM((2 * tok_rows, slots), jnp.bfloat16),
            pltpu.VMEM((tok_rows, tok_rows), jnp.bfloat16),
            pltpu.VMEM((tok_rows, moved_rows), jnp.bfloat16),
            dma((UP_BLOCKS,)),
            dma((DOWN_SLOTS,)),
            dma((7,)),
            dma((CHUNKS,)),
            dma((CHUNKS,)),
            dma((DOWN_BLOCKS,)),
            dma((DOWN_BLOCKS,)),
            dma((2,)),
            dma((2,)),
            dma((MIX_BLOCKS,)),
            dma((MIX_BLOCKS,)),
        ],
        compiler_params=pltpu.CompilerParams(
            collective_id=0, has_side_effects=True, vmem_limit_bytes=KERNEL_VMEM
        ),
        cost_estimate=pl.CostEstimate(
            flops=4 * slots * width * units, bytes_accessed=4 * width * units, transcendentals=slots * units
        ),
    )(*operands)


def finish_kernel(settled, in_moved, received, next_input, new_out, total, store_sem):
    blocks = store_sem.shape[0] - 1
    block_rows = total.shape[0] // blocks
    keep = pltpu.make_async_copy(settled, new_out, store_sem.at[blocks])
    keep.start()
    stores = []
    for b in range(blocks):
        rows = pl.ds(b * block_rows, block_rows)
        total[rows] = (in_moved[rows].astype(jnp.float32) + received[rows].astype(jnp.float32)).astype(jnp.bfloat16)
        stores.append(pltpu.make_async_copy(total.at[rows], next_input.at[rows], store_sem.at[b]))
        stores[-1].start()
    for copy in stores + [keep]:
        copy.wait()


def run_finish_kernel(settled, in_moved, received):
    rows = jax.ShapeDtypeStruct(settled.shape, settled.dtype)
    vmem, anywhere = pl.BlockSpec(memory_space=pltpu.VMEM), pl.BlockSpec(memory_space=pl.ANY)
    return pl.pallas_call(
        finish_kernel,
        out_shape=(rows, rows),
        in_specs=[vmem] * 3,
        out_specs=(anywhere,) * 2,
        scratch_shapes=[pltpu.VMEM(settled.shape, settled.dtype), pltpu.SemaphoreType.DMA((FINISH_BLOCKS + 1,))],
        compiler_params=pltpu.CompilerParams(vmem_limit_bytes=8 * 1024 * 1024),
    )(settled, in_moved, received)


def fits_kernel(tok_rows, width, units, dp_count, expert_count):
    slots = tok_rows * TOPK
    powers = expert_count & (expert_count - 1) == 0
    whole = units % (UP_BLOCKS * 128) == 0 and width % (DOWN_BLOCKS * 128) == 0
    rows = slots % (EXPERTS * CHUNKS * 16) == 0 and tok_rows % 128 == 0
    needed = 2 * (2 * width * units + slots // 2 * (units + units // UP_BLOCKS) + 5 * slots * width)
    return dp_count == 2 and dp_count * expert_count == EXPERTS and powers and whole and rows and needed < DEVICE_VMEM


def per_device(inputs, in_cache, out_cache, w_up, w_down, routing, gate_table, lengths, sample_map):
    tok_rows, width = inputs.shape[1:]
    dp_count = lax.axis_size("dp")
    expert_count = lax.axis_size("expert")
    group_size = dp_count * expert_count
    slice_count = group_size // EXPERTS
    own_dp = lax.axis_index("dp")
    own_device = own_dp * expert_count + lax.axis_index("expert")
    cap_slots = max(1, SAMP_DEV // dp_count)
    per_expert = tok_rows * TOPK // EXPERTS

    if fits_kernel(tok_rows, width, w_up.shape[2], dp_count, expert_count):
        settled, in_moved, received = run_section_kernel(
            routing[0].T, gate_table[0].T, lengths, sample_map,
            inputs[0], in_cache[0], out_cache[0], w_up[0], w_down[0], per_expert,
        )
        next_input, new_out = run_finish_kernel(settled, in_moved, received)
    else:
        select, mix = token_plan(routing[0], gate_table[0], per_expert)
        grouped = jnp.dot(select, inputs[0], preferred_element_type=jnp.float32).astype(jnp.bfloat16)
        grouped = grouped.reshape(EXPERTS, 1, per_expert, width)
        outgoing = jnp.broadcast_to(grouped, (EXPERTS, slice_count, per_expert, width)).reshape(
            group_size, per_expert, width
        )
        arrived = lax.all_to_all(outgoing, ("dp", "expert"), split_axis=0, concat_axis=0, tiled=True)

        to_send, arrival = cache_plan(sample_map, own_device, own_dp, dp_count, expert_count, cap_slots)
        send = jnp.concatenate(
            [
                in_cache[0].reshape(SAMP_DEV, 1, ROWS, width)[to_send],
                out_cache[0].reshape(SAMP_DEV, 1, ROWS, width)[to_send],
            ],
            axis=1,
        )
        send, arrived = lax.optimization_barrier((send, arrived))
        got = lax.all_to_all(send, "dp", split_axis=0, concat_axis=0, tiled=True)

        hidden = jax.nn.silu(
            jnp.dot(arrived.reshape(-1, width), w_up[0], preferred_element_type=jnp.float32)
        ).astype(jnp.bfloat16)
        partial_value = jnp.dot(hidden, w_down[0], preferred_element_type=jnp.float32).astype(jnp.bfloat16)
        returned = lax.all_to_all(
            partial_value.reshape(arrived.shape), ("dp", "expert"), split_axis=0, concat_axis=0, tiled=True
        ).reshape(-1, width)

        mix = jnp.broadcast_to(
            mix.reshape(tok_rows, EXPERTS, 1, per_expert), (tok_rows, EXPERTS, slice_count, per_expert)
        ).reshape(tok_rows, -1)
        high = mix.astype(jnp.bfloat16)
        low = (mix - high.astype(jnp.float32)).astype(jnp.bfloat16)
        both = jnp.dot(jnp.concatenate([high, low], axis=0), returned, preferred_element_type=jnp.float32)
        mixed = both[:tok_rows] + both[tok_rows:]

        in_moved = got[arrival, 0].reshape(tok_rows, width)
        out_moved = got[arrival, 1].reshape(tok_rows, width)

        row_numbers = jnp.arange(tok_rows, dtype=jnp.int32) % ROWS
        valid_rows = row_numbers < jnp.repeat(lengths, ROWS)
        delta_rows = jnp.where(
            valid_rows[:, None],
            (mixed - out_moved.astype(jnp.float32)).astype(jnp.bfloat16),
            jnp.zeros((), jnp.bfloat16),
        )
        received = from_behind(delta_rows, "section", 1)
        new_out = (out_moved.astype(jnp.float32) + delta_rows.astype(jnp.float32)).astype(jnp.bfloat16)
        next_input = (in_moved.astype(jnp.float32) + received.astype(jnp.float32)).astype(jnp.bfloat16)
    return (next_input[None], new_out[None])


def solution(mesh):
    split = P("section", ("dp", "expert"), None)
    placed = (split, split, split, P("section", None, ("dp", "expert")), split, split, split, P(("dp", "expert")), P())
    return jax.shard_map(per_device, mesh=mesh, in_specs=placed, out_specs=(split, split), check_vma=False)
```
